32 devices in a mesh: groups: 2 (over x), seq: 8 (over z, y), section: 2 (over core).
Axes of the slice: x: 2, y: 2, z: 4, core: 2. Of those that a mesh axis runs over, the one named last changes fastest.
Arguments:
- latent_cache: bfloat16 [2, 8, 32768, 576], P('section', 'groups', 'seq'), parts along dimension 1, may hold values from -6 to 6
- index_keys: bfloat16 [2, 8, 32768, 128], P('section', 'groups', 'seq'), parts along dimension 1, may hold values from -6 to 6
- latent_query: bfloat16 [2, 8, 128, 576], P('section', 'groups', 'seq'), parts along dimension 1, may hold values from -54 to 54
- index_query: bfloat16 [2, 8, 64, 128], P('section', 'groups', 'seq'), parts along dimension 1, may hold values from -6 to 6
- index_weight: bfloat16 [2, 8, 64], P('section', 'groups', 'seq'), parts along dimension 1, may hold values from -0.75 to 0.75
- value_up_weight: bfloat16 [2, 128, 512, 128], P('section', 'seq'), may hold values from -0.25 to 0.25
- selected: int32 [2, 8, 2, 32], P('section', 'groups'), parts along dimension 1, may hold values from 0 to 511, as said below
- lengths: int32 [8], P('groups'), parts along dimension 0, may hold values from 16384 to 32767, as said below
Outputs:
- index_scores: float32 [2, 8, 32768], P('section', 'groups', 'seq'), parts along dimension 1
- head_out: bfloat16 [2, 8, 128, 128], P('section', 'groups', 'seq'), parts along dimension 1
The draws below stay inside these ranges and needn't reach their ends.
There are 2 independent parts, one for each index of `groups`. The reference program is written for one: setup_inputs(seed, part) draws one part's arguments, and reference() takes and returns one part's arrays. A program takes and returns all parts, laid end to end along the dimension named above; an argument that names none is the same for every part. Nothing has to cross between parts.
Inputs may be any that keep to these rules, and one draw needn't show every extreme that they name: `lengths`: never one more than a multiple of 64. `selected`: for each layer, row and head group, 32 distinct block numbers, each block starting before the row's length; the block holding the row's last live token is always among them.
All inputs are finite; a program needn't handle non-finite values.
Results may differ from the reference program's by a relative error of at most 0.0048.
Values may be sent and summed in bfloat16 or wider, within the bound.
A program may use at most 128 MiB of HBM per device.

```python
import jax
import jax.numpy as jnp
from jax import lax

ATTENTION_HEADS = 128
LATENT_WIDTH = 512
ROTARY_WIDTH = 64
VALUE_WIDTH = 128
IDX_HEADS = 64
IDX_DIM = 128
BLOCK = 64
HEAD_GROUPS = 2
DECODE_ROWS = 4
CTX_DEV = 4096
CONTEXT_POSITIONS = 32768
LAYER_COUNT = 2
NSEL = 32


def base_lengths(key):
    drawn = jax.random.randint(jax.random.fold_in(key, 11), (DECODE_ROWS,), CONTEXT_POSITIONS // 2, CONTEXT_POSITIONS)
    drawn = jnp.where(drawn % BLOCK == 1, drawn + 1, drawn)
    longest = jax.random.randint(jax.random.fold_in(key, 13), (), 0, DECODE_ROWS)
    row_ids = jnp.arange(DECODE_ROWS, dtype=jnp.int32)
    return jnp.where(row_ids == longest, CONTEXT_POSITIONS - 1, drawn).astype(jnp.int32)


def draw_lengths(key, part):
    return base_lengths(key)


def draw_selected(key, part):
    row_lengths = base_lengths(key)
    count = CONTEXT_POSITIONS // BLOCK
    blocks = jnp.arange(count, dtype=jnp.int32)
    last_block = (row_lengths - 1) // BLOCK
    raw = jax.random.randint(jax.random.fold_in(key, 12), (LAYER_COUNT, DECODE_ROWS, HEAD_GROUPS, count), 0, 2 ** 17)
    ranked = raw * 4096 + blocks
    ranked = jnp.where(blocks[None, None, None, :] <= last_block[None, :, None, None], ranked, -1)
    ranked = jnp.where(blocks[None, None, None, :] == last_block[None, :, None, None], 2 ** 30, ranked)
    return lax.top_k(ranked, NSEL)[1].astype(jnp.int32)


def leading_keys(key):
    width = LATENT_WIDTH + ROTARY_WIDTH
    signs = jax.random.bernoulli(jax.random.fold_in(key, 23), 0.5, (LAYER_COUNT, DECODE_ROWS, width))
    return jnp.where(signs, jnp.float32(1.5), jnp.float32(-1.5))


def latent_values(key):
    width = LATENT_WIDTH + ROTARY_WIDTH
    array_shape = (LAYER_COUNT, DECODE_ROWS, CONTEXT_POSITIONS, width)
    values = jnp.clip(jax.random.normal(jax.random.fold_in(key, 21), array_shape, jnp.float32), -6.0, 6.0)
    row_lengths = base_lengths(key)
    row_ids = jnp.arange(DECODE_ROWS)
    leading = leading_keys(key)
    spread = 0.015 * width ** 0.5
    random_noise = jax.random.normal(jax.random.fold_in(key, 22), (LAYER_COUNT, DECODE_ROWS, width), jnp.float32)
    values = values.at[:, row_ids, row_lengths - 1].set(leading)
    values = values.at[:, row_ids, row_lengths - 2].set(jnp.clip(leading + spread * random_noise, -6.0, 6.0))
    return values


def draw_latent_cache(key, part):
    return latent_values(key).astype(jnp.bfloat16)


def draw_latent_query(key, part):
    width = LATENT_WIDTH + ROTARY_WIDTH
    array_shape = (LAYER_COUNT, DECODE_ROWS, ATTENTION_HEADS, width)
    values = 1.5 * jnp.clip(jax.random.normal(jax.random.fold_in(key, 31), array_shape, jnp.float32), -6.0, 6.0)
    leading = leading_keys(key)
    head_ids = jnp.arange(ATTENTION_HEADS)
    target = jnp.array([120.0, 180.0, 260.0, 340.0], jnp.float32)[head_ids // 8 % 4]
    factor = target / (2.25 * width * (VALUE_WIDTH + ROTARY_WIDTH) ** (-0.5))
    planted = factor[None, None, :, None] * leading[:, :, None, :]
    aligned = (head_ids % 8 == 0)[None, None, :, None]
    values = jnp.where(aligned, planted, values)
    return values.astype(jnp.bfloat16)


def level_of(stream_key, extent, cuts, low, top_value):
    level = 1.0
    for position, parts in cuts:
        heights = jax.random.uniform(jax.random.fold_in(jax.random.fold_in(stream_key, 6), position), (parts,), jnp.float32, low / len(cuts), top_value / len(cuts))
        level = level * jnp.repeat(jnp.exp(heights), extent[position] // parts).reshape((-1,) + (1,) * (len(extent) - 1 - position))
    return level


def normal_values(key, shape, scale, reach, split=(), held_as=jnp.bfloat16):
    values = scale * jax.random.normal(key, shape, jnp.float32)
    if split:
        values = values * level_of(key, shape, split, -0.22, 0.18)
    return jnp.clip(values, -reach, reach).astype(held_as)


def setup_inputs(seed: int = 0, part: int = 0) -> dict:
    splits = jax.random.split(jax.random.key(seed), 9)
    part_keys = jax.random.split(jax.random.fold_in(splits[8], part), 9)
    return {
        "latent_cache": draw_latent_cache(jax.random.fold_in(jax.random.fold_in(splits[8], part), 71), part),
        "index_keys": normal_values(part_keys[1], (LAYER_COUNT, DECODE_ROWS, CONTEXT_POSITIONS, IDX_DIM), 1.0, 6.0, ((0, 2), (2, 8))),
        "latent_query": draw_latent_query(jax.random.fold_in(jax.random.fold_in(splits[8], part), 71), part),
        "index_query": normal_values(part_keys[3], (LAYER_COUNT, DECODE_ROWS, IDX_HEADS, IDX_DIM), 1.0, 6.0, ((0, 2), (2, 8))),
        "index_weight": normal_values(part_keys[4], (LAYER_COUNT, DECODE_ROWS, IDX_HEADS), 0.125, 0.75, ((0, 2), (2, 8))),
        "value_up_weight": normal_values(splits[5], (LAYER_COUNT, ATTENTION_HEADS, LATENT_WIDTH, VALUE_WIDTH), LATENT_WIDTH ** -0.5, 0.25, ((0, 2), (1, 8))),
        "selected": draw_selected(jax.random.fold_in(jax.random.fold_in(splits[8], part), 71), part),
        "lengths": draw_lengths(jax.random.fold_in(jax.random.fold_in(splits[8], part), 71), part),
    }


def reference(latent_cache, index_keys, latent_query, index_query, index_weight, value_up_weight, selected, lengths):
    scale = (VALUE_WIDTH + ROTARY_WIDTH) ** -0.5
    positions = jnp.arange(CONTEXT_POSITIONS, dtype=jnp.int32)
    live_mask = positions[None, :] < lengths[:, None]
    group_wise = ATTENTION_HEADS // HEAD_GROUPS
    spans = CONTEXT_POSITIONS // CTX_DEV
    score_list = []
    head_list = []
    for layer_index in range(LAYER_COUNT):
        index_dots = jnp.einsum("bhd,btd->bht", index_query[layer_index].astype(jnp.float32), index_keys[layer_index].astype(jnp.float32))
        weighted = jax.nn.relu(index_dots * IDX_DIM ** -0.5) * index_weight[layer_index].astype(jnp.float32)[:, :, None]
        score_list.append(jnp.where(live_mask, jnp.sum(weighted, axis=1), jnp.float32(0.0)))

        def one_row(packed):
            latent_rows, query_matrix, chosen, row_length = packed
            tokens = (chosen[:, :, None] * BLOCK + jnp.arange(BLOCK, dtype=jnp.int32)[None, None, :]).reshape(HEAD_GROUPS, NSEL * BLOCK).astype(jnp.int32)
            picked_blocks = latent_rows[tokens].astype(jnp.float32)
            group_split = query_matrix.reshape(HEAD_GROUPS, group_wise, LATENT_WIDTH + ROTARY_WIDTH).astype(jnp.float32)
            scores = jnp.einsum("ghd,gkd->ghk", group_split, picked_blocks) * scale
            usable = (tokens < row_length)[:, None, :]
            masked = jnp.where(usable, scores, jnp.float32(-1e30))
            shard = (tokens // CTX_DEV).astype(jnp.int32)
            onehot = shard[:, None, :, None] == jnp.arange(spans, dtype=jnp.int32)[None, None, None, :]
            shard_max = jnp.max(jnp.where(onehot, masked[..., None], jnp.float32(-1e30)), axis=2)
            local_max = jnp.take_along_axis(shard_max, jnp.broadcast_to(shard[:, None, :], masked.shape).astype(jnp.int32), axis=2)
            row_max = jnp.max(shard_max, axis=2, keepdims=True)
            local_weights = jnp.where(usable, jnp.exp(masked - local_max), jnp.float32(0.0))
            factor = jnp.where(usable, jnp.exp(local_max - row_max), jnp.float32(0.0))
            total_per_row = jnp.sum(local_weights * factor, axis=2)
            rounded_values = local_weights.astype(jnp.bfloat16).astype(jnp.float32) * factor
            summed_values = jnp.einsum("qyj,qjp->qyp", rounded_values, picked_blocks[:, :, :LATENT_WIDTH])
            return (summed_values / total_per_row[:, :, None]).astype(jnp.bfloat16).reshape(ATTENTION_HEADS, LATENT_WIDTH)

        attended = lax.map(one_row, (latent_cache[layer_index], latent_query[layer_index], selected[layer_index], lengths))
        projected = jnp.einsum("bhc,hcv->bhv", attended.astype(jnp.float32), value_up_weight[layer_index].astype(jnp.float32))
        head_list.append(projected.astype(jnp.bfloat16))
    return jnp.stack(score_list), jnp.stack(head_list)
```

```python
import functools

import jax
import jax.numpy as jnp
from jax import lax
from jax.experimental import pallas as pl
from jax.experimental.pallas import tpu as pltpu
from jax.sharding import PartitionSpec as P

LATENT_WIDTH = 512
ROTARY_WIDTH = 64
VALUE_WIDTH = 128
IDX_DIM = 128
BLOCK = 64
HEAD_GROUPS = 2
NEG = -1e30
CHUNK = 8
LANES = 128
MESH = pl.DeviceIdType.MESH


def greet_all(n, me):
    barrier = pltpu.get_barrier_semaphore()
    for k in range(1, n):
        pl.semaphore_signal(
            barrier, inc=1, device_id={"seq": lax.rem(me + k, n)}, device_id_type=MESH
        )
    pl.semaphore_wait(barrier, n - 1)


def push(n, me, k, src, dst, send_sem, recv_sem):
    return pltpu.make_async_remote_copy(
        src_ref=src,
        dst_ref=dst,
        send_sem=send_sem.at[k],
        recv_sem=recv_sem.at[k],
        device_id={"seq": lax.rem(me + k, n)},
        device_id_type=MESH,
    )


def gather_kernel(
    n, lens, lq, iqx, keys, gq, scores, giq, kbuf,
    key_sem, own_sem, isend, irecv, qsend, qrecv,
):
    me = lax.axis_index("seq")
    rows, span, _ = keys.shape
    loads = []
    for b in range(rows):
        copy = pltpu.make_async_copy(keys.at[b], kbuf.at[b], key_sem.at[b])
        copy.start()
        loads.append(copy)
    own = [
        pltpu.make_async_copy(iqx, giq.at[me], own_sem.at[0]),
        pltpu.make_async_copy(lq, gq.at[me], own_sem.at[1]),
    ]
    for copy in own:
        copy.start()
    greet_all(n, me)
    small = [push(n, me, k, iqx, giq.at[me], isend, irecv) for k in range(1, n)]
    large = [push(n, me, k, lq, gq.at[me], qsend, qrecv) for k in range(1, n)]
    for copy in small:
        copy.start()
    for copy in large:
        copy.start()
    for copy in loads:
        copy.wait()
    own[0].wait()
    for copy in small:
        copy.wait_recv()
    tile = min(512, span)
    lane = lax.broadcasted_iota(jnp.int32, (1, tile), 1)
    for b in range(rows):
        packed = giq[:, b].astype(jnp.float32)
        packed = packed.reshape(packed.shape[0] * packed.shape[1], packed.shape[2])
        query = packed[:, :IDX_DIM].astype(jnp.bfloat16)
        weight = packed[:, IDX_DIM:] * IDX_DIM ** (-0.5)
        length = lens[b]

        def step(c, carry, b=b, query=query, weight=weight, length=length):
            start = pl.multiple_of(c * tile, tile)
            dots = lax.dot_general(
                query,
                kbuf[b, pl.ds(start, tile), :],
                (((1,), (1,)), ((), ())),
                preferred_element_type=jnp.float32,
            )
            pieces = []
            for j in range(tile // 128):
                part = jnp.maximum(dots[:, j * 128 : (j + 1) * 128], 0.0) * weight
                pieces.append(jnp.sum(part, axis=0, keepdims=True))
            total = jnp.concatenate(pieces, axis=1)
            live = me * span + c * tile + lane < length
            scores[b : b + 1, pl.ds(start, tile)] = jnp.where(live, total, 0.0)
            return carry

        lax.fori_loop(0, span // tile, step, 0)
    own[1].wait()
    for copy in large:
        copy.wait_recv()
    for copy in small + large:
        copy.wait_send()


def local_kernel(sel, lens, gq, cache, parts, stats, buf, counts, low, high, sems):
    me = lax.axis_index("seq")
    rows, width, span = cache.shape
    nsel = sel.shape[2]
    here = span // BLOCK
    first = me * here

    def block_copy(b, rg, block, slot):
        start = pl.multiple_of((block - first) // 2 * LANES, LANES)
        dest = pl.multiple_of(slot * LANES, LANES)
        return pltpu.make_async_copy(
            cache.at[b, :, pl.ds(start, LANES)],
            buf.at[rg, :, pl.ds(dest, LANES)],
            sems.at[rg, slot],
        )

    for b in range(rows):
        for g in range(HEAD_GROUPS):
            rg = b * HEAD_GROUPS + g

            def scan(i, slot, b=b, g=g, rg=rg):
                block = sel[b, g, i]
                mine = jnp.logical_and(block >= first, block < first + here)

                @pl.when(mine)
                def _():
                    block_copy(b, rg, block, slot).start()
                    begin = block % 2 * BLOCK
                    low[rg, slot] = begin
                    high[rg, slot] = begin + jnp.minimum(BLOCK, lens[b] - block * BLOCK)

                return slot + mine.astype(jnp.int32)

            counts[rg] = lax.fori_loop(0, nsel, scan, jnp.int32(0), unroll=4)

    heads = gq.shape[2]
    per_group = gq.shape[0] // HEAD_GROUPS
    group_wise = per_group * heads
    tokens = CHUNK * LANES
    scale = (VALUE_WIDTH + ROTARY_WIDTH) ** (-0.5)
    lane = lax.broadcasted_iota(jnp.int32, (1, LANES), 1)
    for g in range(HEAD_GROUPS):
        table = jnp.zeros((group_wise, LANES), jnp.float32)
        for b in range(rows):
            rg = b * HEAD_GROUPS + g
            count = counts[rg]
            steps = jnp.maximum((count + CHUNK - 1) // CHUNK, 1)

            @pl.loop(count, steps * CHUNK)
            def _(slot, rg=rg):
                dest = pl.multiple_of(slot * LANES, LANES)
                buf[rg, :, pl.ds(dest, LANES)] = jnp.zeros((width, LANES), jnp.bfloat16)
                low[rg, slot] = 0
                high[rg, slot] = 0

            @pl.loop(0, count)
            def _(slot, b=b, rg=rg):
                block_copy(b, rg, first, slot).wait()

            query = gq[g * per_group : (g + 1) * per_group, b].reshape(group_wise, width)

            def chunk(c, rg=rg, query=query):
                base = pl.multiple_of(c * tokens, tokens)
                s = jnp.dot(
                    query,
                    buf[rg, :, pl.ds(base, tokens)],
                    preferred_element_type=jnp.float32,
                ) * scale
                bounds = [
                    (low[rg, c * CHUNK + j], high[rg, c * CHUNK + j]) for j in range(CHUNK)
                ]
                usable = jnp.concatenate(
                    [
                        ((lane >= lo) & (lane < hi)).astype(jnp.int32)
                        for lo, hi in bounds
                    ],
                    axis=1,
                ) > 0
                s = jnp.where(usable, s, NEG)
                return s, usable, buf[rg, :LATENT_WIDTH, pl.ds(base, tokens)]

            def mix(p, values):
                return lax.dot_general(
                    p.astype(jnp.bfloat16),
                    values,
                    (((1,), (1,)), ((), ())),
                    preferred_element_type=jnp.float32,
                )

            s, usable, values = chunk(0)
            top = jnp.max(s, axis=1, keepdims=True)
            p = jnp.where(usable, jnp.exp(s - top), 0.0)
            total = jnp.sum(p, axis=1, keepdims=True)
            acc = mix(p, values)

            def more(c, carry, chunk=chunk):
                top, total, acc = carry
                s, usable, values = chunk(c)
                new = jnp.maximum(top, jnp.max(s, axis=1, keepdims=True))
                p = jnp.where(usable, jnp.exp(s - new), 0.0)
                keep = jnp.exp(top - new)
                total = total * keep + jnp.sum(p, axis=1, keepdims=True)
                return new, total, acc * keep + mix(p, values)

            top, total, acc = lax.fori_loop(1, steps, more, (top, total, acc))
            parts[g * per_group : (g + 1) * per_group, b] = acc.astype(jnp.bfloat16).reshape(
                per_group, heads, LATENT_WIDTH
            )
            table = jnp.where(lane == 2 * b, top, table)
            table = jnp.where(lane == 2 * b + 1, total, table)
        stats[g * per_group : (g + 1) * per_group] = table.reshape(per_group, heads, LANES)


def exchange_kernel(
    n, parts, stats, weight, out, rparts, rstats, wbuf,
    own_sem, psend, precv, ssend, srecv,
):
    me = lax.axis_index("seq")
    _, rows, heads, latent = parts.shape
    own = [
        pltpu.make_async_copy(weight, wbuf, own_sem.at[0]),
        pltpu.make_async_copy(parts.at[me], rparts.at[me], own_sem.at[1]),
        pltpu.make_async_copy(stats.at[me], rstats.at[me], own_sem.at[2]),
    ]
    for copy in own:
        copy.start()
    greet_all(n, me)
    sends = []
    for k in range(1, n):
        peer = lax.rem(me + k, n)
        sends.append(push(n, me, k, stats.at[peer], rstats.at[me], ssend, srecv))
        sends.append(push(n, me, k, parts.at[peer], rparts.at[me], psend, precv))
    for copy in sends:
        copy.start()
    for copy in own:
        copy.wait()
    for copy in sends:
        copy.wait_recv()
    table = rstats[...]
    attended = []
    for b in range(rows):
        tops = [table[s, :, 2 * b : 2 * b + 1] for s in range(n)]
        joint = functools.reduce(jnp.maximum, tops)
        total = jnp.zeros_like(joint)
        acc = jnp.zeros((heads, latent), jnp.float32)
        for s in range(n):
            factor = jnp.exp(tops[s] - joint)
            total = total + factor * table[s, :, 2 * b + 1 : 2 * b + 2]
            acc = acc + factor * rparts[s, b].astype(jnp.float32)
        attended.append(acc / total)
    attended = jnp.concatenate(attended, axis=0).astype(jnp.bfloat16)
    which = lax.broadcasted_iota(jnp.int32, (rows * heads, 1), 0) % heads

    def project(h, acc):
        y = jnp.dot(attended, wbuf[h], preferred_element_type=jnp.float32)
        return jnp.where(which == h, y, acc)

    y = jnp.zeros((rows * heads, weight.shape[2]), jnp.float32)
    y = lax.fori_loop(0, heads, project, y, unroll=4)
    out[...] = y.reshape(rows, heads, weight.shape[2]).astype(out.dtype)
    for copy in sends:
        copy.wait_send()


def on_device(
    n,
    latent_cache,
    index_keys,
    latent_query,
    index_query,
    index_weight,
    value_up_weight,
    selected,
    lengths,
):
    cache, keys, lq = latent_cache[0], index_keys[0], latent_query[0]
    iq, iw, weight, sel = index_query[0], index_weight[0], value_up_weight[0], selected[0]
    rows, span, width = cache.shape
    heads = lq.shape[1]
    extra = -iq.shape[1] % 8
    iqx = jnp.concatenate(
        [iq, jnp.broadcast_to(iw[:, :, None], iw.shape + (128,))], axis=2
    )
    iqx = jnp.pad(iqx, ((0, 0), (0, extra), (0, 0)))
    vmem = pl.BlockSpec(memory_space=pltpu.VMEM)
    smem = pl.BlockSpec(memory_space=pltpu.SMEM)
    hbm = pl.BlockSpec(memory_space=pl.ANY)
    dma = pltpu.SemaphoreType.DMA
    limit = 60 * 1024 * 1024

    gq, index_scores = pl.pallas_call(
        functools.partial(gather_kernel, n),
        out_shape=(
            jax.ShapeDtypeStruct((n,) + lq.shape, lq.dtype),
            jax.ShapeDtypeStruct((rows, span), jnp.float32),
        ),
        in_specs=[smem, vmem, vmem, hbm],
        out_specs=(hbm, vmem),
        scratch_shapes=[
            pltpu.VMEM((n,) + iqx.shape, iqx.dtype),
            pltpu.VMEM(keys.shape, keys.dtype),
            dma((rows,)), dma((2,)), dma((n,)), dma((n,)), dma((n,)), dma((n,)),
        ],
        compiler_params=pltpu.CompilerParams(
            collective_id=0, has_side_effects=True, vmem_limit_bytes=limit
        ),
        name="gather",
    )(lengths, lq, iqx, keys)

    whole_heads = n * heads
    if heads % 16:
        gq = gq.transpose(1, 0, 2, 3).reshape(
            rows, HEAD_GROUPS, whole_heads // HEAD_GROUPS, width
        ).transpose(1, 0, 2, 3)
    slots = gq.shape[0]
    wide = gq.shape[2]
    pairs = rows * HEAD_GROUPS
    nsel = sel.shape[2]
    room = -(-nsel // CHUNK) * CHUNK
    parts, stats = pl.pallas_call(
        local_kernel,
        out_shape=(
            jax.ShapeDtypeStruct((slots, rows, wide, LATENT_WIDTH), jnp.bfloat16),
            jax.ShapeDtypeStruct((slots, wide, 128), jnp.float32),
        ),
        in_specs=[smem, smem, vmem, hbm],
        out_specs=(vmem, vmem),
        scratch_shapes=[
            pltpu.VMEM((pairs, width, room * LANES), cache.dtype),
            pltpu.SMEM((pairs,), jnp.int32),
            pltpu.SMEM((pairs, room), jnp.int32),
            pltpu.SMEM((pairs, room), jnp.int32),
            dma((pairs, nsel)),
        ],
        compiler_params=pltpu.CompilerParams(vmem_limit_bytes=limit),
        name="local",
    )(sel, lengths, gq, jnp.swapaxes(cache, 1, 2))
    if slots != n:
        parts = parts.transpose(1, 0, 2, 3).reshape(rows, n, heads, LATENT_WIDTH)
        parts = parts.transpose(1, 0, 2, 3)
        stats = stats.reshape(n, heads, 128)

    head_out = pl.pallas_call(
        functools.partial(exchange_kernel, n),
        out_shape=jax.ShapeDtypeStruct((rows, heads, weight.shape[2]), jnp.bfloat16),
        in_specs=[hbm, hbm, hbm],
        out_specs=vmem,
        scratch_shapes=[
            pltpu.VMEM(parts.shape, parts.dtype),
            pltpu.VMEM(stats.shape, stats.dtype),
            pltpu.VMEM(weight.shape, weight.dtype),
            dma((3,)), dma((n,)), dma((n,)), dma((n,)), dma((n,)),
        ],
        compiler_params=pltpu.CompilerParams(
            collective_id=1, has_side_effects=True, vmem_limit_bytes=limit
        ),
        name="exchange",
    )(parts, stats, weight)
    return (index_scores[None], head_out[None])


def solution(mesh):
    return jax.shard_map(
        functools.partial(on_device, mesh.shape["seq"]),
        mesh=mesh,
        in_specs=(
            P("section", "groups", "seq", None),
            P("section", "groups", "seq", None),
            P("section", "groups", "seq", None),
            P("section", "groups", "seq", None),
            P("section", "groups", "seq"),
            P("section", "seq", None, None),
            P("section", "groups", None, None),
            P("groups"),
        ),
        out_specs=(P("section", "groups", "seq"), P("section", "groups", "seq", None)),
        check_vma=False,
    )
```

```python
import functools

import jax
import jax.numpy as jnp
from jax import lax
from jax.experimental import pallas as pl
from jax.experimental.pallas import tpu as pltpu
from jax.sharding import PartitionSpec as P

LATENT_WIDTH = 512
ROTARY_WIDTH = 64
VALUE_WIDTH = 128
IDX_DIM = 128
BLOCK = 64
HEAD_GROUPS = 2
NEG = -1e30
CHUNK = 8
LANES = 128
MESH = pl.DeviceIdType.MESH


def greet_all(n, me):
    barrier = pltpu.get_barrier_semaphore()
    for k in range(1, n):
        pl.semaphore_signal(
            barrier, inc=1, device_id={"seq": lax.rem(me + k, n)}, device_id_type=MESH
        )
    pl.semaphore_wait(barrier, n - 1)


def push(n, me, k, src, dst, send_sem, recv_sem):
    return pltpu.make_async_remote_copy(
        src_ref=src,
        dst_ref=dst,
        send_sem=send_sem.at[k],
        recv_sem=recv_sem.at[k],
        device_id={"seq": lax.rem(me + k, n)},
        device_id_type=MESH,
    )


def gather_kernel(
    n, lens, lq, iq, iw, keys, gq, scores, giq, giw, kbuf,
    key_sem, own_sem, isend, irecv, wsend, wrecv, qsend, qrecv,
):
    me = lax.axis_index("seq")
    rows, span, _ = keys.shape
    half = n // 2
    partner = me + 1 - 2 * lax.rem(me, 2)
    order = sorted(range(1, half), key=lambda k: min(k, half - k))
    loads = []
    for b in range(rows):
        copy = pltpu.make_async_copy(keys.at[b], kbuf.at[b], key_sem.at[b])
        copy.start()
        loads.append(copy)
    own = [
        pltpu.make_async_copy(iq, giq.at[me], own_sem.at[0]),
        pltpu.make_async_copy(iw, giw.at[me], own_sem.at[1]),
        pltpu.make_async_copy(lq, gq.at[me], own_sem.at[2]),
    ]
    for copy in own:
        copy.start()
    greet_all(n, me)

    def push(peer, k, src, dst, send_sem, recv_sem):
        return pltpu.make_async_remote_copy(
            src_ref=src,
            dst_ref=dst,
            send_sem=send_sem.at[k],
            recv_sem=recv_sem.at[k],
            device_id={"seq": peer},
            device_id_type=MESH,
        )

    def first_hop(src, dst, send_sem, recv_sem):
        away = {
            k: push(lax.rem(me + 2 * k, n), k, src, dst.at[me], send_sem, recv_sem)
            for k in order
        }
        return away, push(partner, half, src, dst.at[me], send_sem, recv_sem)

    def second_hop(dst, send_sem, recv_sem):
        passed = {}
        for k in order:
            owner = lax.rem(me - 2 * k + n, n)
            passed[k] = push(
                partner, half + k, dst.at[owner], dst.at[owner], send_sem, recv_sem
            )
        return passed

    small = [(iq, giq, isend, irecv), (iw, giw, wsend, wrecv)]
    small_hops = [(first_hop(*x), second_hop(*x[1:])) for x in small]
    (large, large_pair), large_on = first_hop(lq, gq, qsend, qrecv), second_hop(gq, qsend, qrecv)
    for (away, pair), _ in small_hops:
        for k in order:
            away[k].start()
        pair.start()
    for k in order:
        large[k].start()
    large_pair.start()
    for (away, _), passed in small_hops:
        for k in order:
            away[k].wait_recv()
            passed[k].start()
    for copy in loads:
        copy.wait()
    own[0].wait()
    own[1].wait()
    for (_, pair), passed in small_hops:
        pair.wait_recv()
        for k in order:
            passed[k].wait_recv()
    tile = min(512, span)
    lane = lax.broadcasted_iota(jnp.int32, (1, tile), 1)
    held = giq.shape[2]
    given = iw.shape[1]
    diagonal = (
        lax.broadcasted_iota(jnp.int32, (n * held, given), 0) % held
        == lax.broadcasted_iota(jnp.int32, (n * held, given), 1)
    )
    waiting = list(order)
    for b in range(rows):
        query = giq[:, b].astype(jnp.float32).reshape(n * held, giq.shape[3])
        query = query.astype(jnp.bfloat16)
        weight = giw[:, b : b + 1].astype(jnp.float32)
        weight = jnp.broadcast_to(weight, (n, held, given)).reshape(n * held, given)
        weight = jnp.sum(jnp.where(diagonal, weight, 0.0), axis=1, keepdims=True)
        weight = jnp.broadcast_to(weight * IDX_DIM ** (-0.5), (n * held, LANES))
        length = lens[b]

        def step(c, carry, b=b, query=query, weight=weight, length=length):
            start = pl.multiple_of(c * tile, tile)
            dots = lax.dot_general(
                query,
                kbuf[b, pl.ds(start, tile), :],
                (((1,), (1,)), ((), ())),
                preferred_element_type=jnp.float32,
            )
            pieces = []
            for j in range(tile // LANES):
                part = jnp.maximum(dots[:, j * LANES : (j + 1) * LANES], 0.0) * weight
                pieces.append(jnp.sum(part, axis=0, keepdims=True))
            total = jnp.concatenate(pieces, axis=1)
            live = me * span + c * tile + lane < length
            scores[b : b + 1, pl.ds(start, tile)] = jnp.where(live, total, 0.0)
            return carry

        lax.fori_loop(0, span // tile, step, 0)
        if waiting:
            k = waiting.pop(0)
            large[k].wait_recv()
            large_on[k].start()
    for k in waiting:
        large[k].wait_recv()
        large_on[k].start()
    own[2].wait()
    large_pair.wait_recv()
    for k in order:
        large_on[k].wait_recv()
    for (away, pair), passed in small_hops + [((large, large_pair), large_on)]:
        pair.wait_send()
        for k in order:
            away[k].wait_send()
            passed[k].wait_send()


def local_kernel(sel, lens, gq, cache, parts, stats, buf, counts, kept, sems):
    me = lax.axis_index("seq")
    rows, width, span = cache.shape
    nsel = sel.shape[2]
    here = span // BLOCK
    first = me * here

    def block_copy(b, rg, block, slot):
        start = pl.multiple_of((block - first) // 2 * LANES, LANES)
        dest = pl.multiple_of(slot * LANES, LANES)
        return pltpu.make_async_copy(
            cache.at[b, :, pl.ds(start, LANES)],
            buf.at[rg, :, pl.ds(dest, LANES)],
            sems.at[rg, slot],
        )

    for b in range(rows):
        for g in range(HEAD_GROUPS):
            rg = b * HEAD_GROUPS + g

            def scan(i, slot, b=b, g=g, rg=rg):
                block = sel[b, g, i]
                kept[rg, slot] = block
                mine = jnp.logical_and(block >= first, block < first + here)
                return slot + mine.astype(jnp.int32)

            count = lax.fori_loop(0, nsel, scan, jnp.int32(0), unroll=True)
            counts[rg] = count

            @pl.loop(0, count)
            def _(slot, b=b, rg=rg):
                block_copy(b, rg, kept[rg, slot], slot).start()

    for rg in range(rows * HEAD_GROUPS):
        count = counts[rg]

        @pl.loop(count, jnp.maximum((count + CHUNK - 1) // CHUNK, 1) * CHUNK)
        def _(slot, rg=rg):
            dest = pl.multiple_of(slot * LANES, LANES)
            buf[rg, :, pl.ds(dest, LANES)] = jnp.zeros((width, LANES), jnp.bfloat16)

    heads = gq.shape[2]
    per_group = gq.shape[0] // HEAD_GROUPS
    group_wise = per_group * heads
    tokens = CHUNK * LANES
    scale = (VALUE_WIDTH + ROTARY_WIDTH) ** (-0.5)
    lane = lax.broadcasted_iota(jnp.int32, (1, LANES), 1)
    for g in range(HEAD_GROUPS):
        table = jnp.zeros((group_wise, LANES), jnp.float32)
        for b in range(rows):
            rg = b * HEAD_GROUPS + g
            count = counts[rg]
            steps = jnp.maximum((count + CHUNK - 1) // CHUNK, 1)

            @pl.loop(0, count)
            def _(slot, b=b, rg=rg):
                block_copy(b, rg, first, slot).wait()

            query = gq[g * per_group : (g + 1) * per_group, b].reshape(group_wise, width)

            def chunk(c, b=b, rg=rg, query=query, count=count):
                base = pl.multiple_of(c * tokens, tokens)
                s = jnp.dot(
                    query,
                    buf[rg, :, pl.ds(base, tokens)],
                    preferred_element_type=jnp.float32,
                ) * scale
                bounds = []
                for j in range(CHUNK):
                    slot = c * CHUNK + j
                    block = kept[rg, slot]
                    begin = block % 2 * BLOCK
                    live = jnp.minimum(BLOCK, lens[b] - block * BLOCK)
                    bounds.append((begin, jnp.where(slot < count, begin + live, 0)))
                usable = jnp.concatenate(
                    [
                        ((lane >= lo) & (lane < hi)).astype(jnp.int32)
                        for lo, hi in bounds
                    ],
                    axis=1,
                ) > 0
                s = jnp.where(usable, s, NEG)
                return s, usable, buf[rg, :LATENT_WIDTH, pl.ds(base, tokens)]

            def mix(p, values):
                return lax.dot_general(
                    p.astype(jnp.bfloat16),
                    values,
                    (((1,), (1,)), ((), ())),
                    preferred_element_type=jnp.float32,
                )

            s, usable, values = chunk(0)
            top = jnp.max(s, axis=1, keepdims=True)
            p = jnp.where(usable, jnp.exp(s - top), 0.0)
            total = jnp.sum(p, axis=1, keepdims=True)
            acc = mix(p, values)

            def more(c, carry, chunk=chunk):
                top, total, acc = carry
                s, usable, values = chunk(c)
                new = jnp.maximum(top, jnp.max(s, axis=1, keepdims=True))
                p = jnp.where(usable, jnp.exp(s - new), 0.0)
                keep = jnp.exp(top - new)
                total = total * keep + jnp.sum(p, axis=1, keepdims=True)
                return new, total, acc * keep + mix(p, values)

            top, total, acc = lax.fori_loop(1, steps, more, (top, total, acc))
            parts[g * per_group : (g + 1) * per_group, b] = acc.astype(jnp.bfloat16).reshape(
                per_group, heads, LATENT_WIDTH
            )
            table = jnp.where(lane == 2 * b, top, table)
            table = jnp.where(lane == 2 * b + 1, total, table)
        stats[g * per_group : (g + 1) * per_group] = table.reshape(per_group, heads, LANES)


def exchange_kernel(
    n, parts, stats, weight, out, rparts, rstats, wbuf,
    own_sem, psend, precv, ssend, srecv,
):
    me = lax.axis_index("seq")
    _, rows, heads, latent = parts.shape
    own = [
        pltpu.make_async_copy(weight, wbuf, own_sem.at[0]),
        pltpu.make_async_copy(parts.at[me], rparts.at[me], own_sem.at[1]),
        pltpu.make_async_copy(stats.at[me], rstats.at[me], own_sem.at[2]),
    ]
    for copy in own:
        copy.start()
    greet_all(n, me)
    sends = []
    for k in range(1, n):
        peer = lax.rem(me + k, n)
        sends.append(push(n, me, k, stats.at[peer], rstats.at[me], ssend, srecv))
        sends.append(push(n, me, k, parts.at[peer], rparts.at[me], psend, precv))
    for copy in sends:
        copy.start()
    for copy in own:
        copy.wait()
    for copy in sends:
        copy.wait_recv()
    table = rstats[...]
    attended = []
    for b in range(rows):
        tops = [table[s, :, 2 * b : 2 * b + 1] for s in range(n)]
        joint = functools.reduce(jnp.maximum, tops)
        total = jnp.zeros_like(joint)
        acc = jnp.zeros((heads, latent), jnp.float32)
        for s in range(n):
            factor = jnp.exp(tops[s] - joint)
            total = total + factor * table[s, :, 2 * b + 1 : 2 * b + 2]
            acc = acc + factor * rparts[s, b].astype(jnp.float32)
        attended.append(acc / total)
    attended = jnp.concatenate(attended, axis=0).astype(jnp.bfloat16)
    which = lax.broadcasted_iota(jnp.int32, (rows * heads, 1), 0) % heads

    def project(h, acc):
        y = jnp.dot(attended, wbuf[h], preferred_element_type=jnp.float32)
        return jnp.where(which == h, y, acc)

    y = jnp.zeros((rows * heads, weight.shape[2]), jnp.float32)
    y = lax.fori_loop(0, heads, project, y, unroll=4)
    out[...] = y.reshape(rows, heads, weight.shape[2]).astype(out.dtype)
    for copy in sends:
        copy.wait_send()


def on_device(
    n,
    latent_cache,
    index_keys,
    latent_query,
    index_query,
    index_weight,
    value_up_weight,
    selected,
    lengths,
):
    cache, keys, lq = latent_cache[0], index_keys[0], latent_query[0]
    iq, iw, weight, sel = index_query[0], index_weight[0], value_up_weight[0], selected[0]
    rows, span, width = cache.shape
    heads = lq.shape[1]
    extra = -iq.shape[1] % 8
    if extra:
        iq = jnp.pad(iq, ((0, 0), (0, extra), (0, 0)))
    vmem = pl.BlockSpec(memory_space=pltpu.VMEM)
    smem = pl.BlockSpec(memory_space=pltpu.SMEM)
    hbm = pl.BlockSpec(memory_space=pl.ANY)
    dma = pltpu.SemaphoreType.DMA
    limit = 60 * 1024 * 1024

    gq, index_scores = pl.pallas_call(
        functools.partial(gather_kernel, n),
        out_shape=(
            jax.ShapeDtypeStruct((n,) + lq.shape, lq.dtype),
            jax.ShapeDtypeStruct((rows, span), jnp.float32),
        ),
        in_specs=[smem, vmem, vmem, vmem, hbm],
        out_specs=(hbm, vmem),
        scratch_shapes=[
            pltpu.VMEM((n,) + iq.shape, iq.dtype),
            pltpu.VMEM((n,) + iw.shape, iw.dtype),
            pltpu.VMEM(keys.shape, keys.dtype),
            dma((rows,)), dma((3,)), dma((n,)), dma((n,)), dma((n,)), dma((n,)),
            dma((n,)), dma((n,)),
        ],
        compiler_params=pltpu.CompilerParams(
            collective_id=0, has_side_effects=True, vmem_limit_bytes=limit
        ),
        name="gather",
    )(lengths, lq, iq, iw, keys)

    whole_heads = n * heads
    if heads % 16:
        gq = gq.transpose(1, 0, 2, 3).reshape(
            rows, HEAD_GROUPS, whole_heads // HEAD_GROUPS, width
        ).transpose(1, 0, 2, 3)
    slots = gq.shape[0]
    wide = gq.shape[2]
    pairs = rows * HEAD_GROUPS
    nsel = sel.shape[2]
    room = -(-nsel // CHUNK) * CHUNK
    parts, stats = pl.pallas_call(
        local_kernel,
        out_shape=(
            jax.ShapeDtypeStruct((slots, rows, wide, LATENT_WIDTH), jnp.bfloat16),
            jax.ShapeDtypeStruct((slots, wide, 128), jnp.float32),
        ),
        in_specs=[smem, smem, vmem, hbm],
        out_specs=(vmem, vmem),
        scratch_shapes=[
            pltpu.VMEM((pairs, width, room * LANES), cache.dtype),
            pltpu.SMEM((pairs,), jnp.int32),
            pltpu.SMEM((pairs, room), jnp.int32),
            dma((pairs, nsel)),
        ],
        compiler_params=pltpu.CompilerParams(vmem_limit_bytes=limit),
        name="local",
    )(sel, lengths, gq, jnp.swapaxes(cache, 1, 2))
    if slots != n:
        parts = parts.transpose(1, 0, 2, 3).reshape(rows, n, heads, LATENT_WIDTH)
        parts = parts.transpose(1, 0, 2, 3)
        stats = stats.reshape(n, heads, 128)

    head_out = pl.pallas_call(
        functools.partial(exchange_kernel, n),
        out_shape=jax.ShapeDtypeStruct((rows, heads, weight.shape[2]), jnp.bfloat16),
        in_specs=[hbm, hbm, hbm],
        out_specs=vmem,
        scratch_shapes=[
            pltpu.VMEM(parts.shape, parts.dtype),
            pltpu.VMEM(stats.shape, stats.dtype),
            pltpu.VMEM(weight.shape, weight.dtype),
            dma((3,)), dma((n,)), dma((n,)), dma((n,)), dma((n,)),
        ],
        compiler_params=pltpu.CompilerParams(
            collective_id=1, has_side_effects=True, vmem_limit_bytes=limit
        ),
        name="exchange",
    )(parts, stats, weight)
    return (index_scores[None], head_out[None])


def solution(mesh):
    return jax.shard_map(
        functools.partial(on_device, mesh.shape["seq"]),
        mesh=mesh,
        in_specs=(
            P("section", "groups", "seq", None),
            P("section", "groups", "seq", None),
            P("section", "groups", "seq", None),
            P("section", "groups", "seq", None),
            P("section", "groups", "seq"),
            P("section", "seq", None, None),
            P("section", "groups", None, None),
            P("groups"),
        ),
        out_specs=(P("section", "groups", "seq"), P("section", "groups", "seq", None)),
        check_vma=False,
    )
```

```python
import functools

import jax
import jax.numpy as jnp
from jax import lax
from jax.experimental import pallas as pl
from jax.experimental.pallas import tpu as pltpu
from jax.sharding import PartitionSpec as P

LATENT_WIDTH = 512
ROTARY_WIDTH = 64
VALUE_WIDTH = 128
IDX_DIM = 128
BLOCK = 64
HEAD_GROUPS = 2
NEG = -1e30
CHUNK = 8
LANES = 128
MESH = pl.DeviceIdType.MESH


def greet_all(n, me):
    barrier = pltpu.get_barrier_semaphore()
    for k in range(1, n):
        pl.semaphore_signal(
            barrier, inc=1, device_id={"seq": lax.rem(me + k, n)}, device_id_type=MESH
        )
    pl.semaphore_wait(barrier, n - 1)


def push(n, me, k, src, dst, send_sem, recv_sem):
    return pltpu.make_async_remote_copy(
        src_ref=src,
        dst_ref=dst,
        send_sem=send_sem.at[k],
        recv_sem=recv_sem.at[k],
        device_id={"seq": lax.rem(me + k, n)},
        device_id_type=MESH,
    )


def gather_kernel(
    n, lens, lq, iq, iw, keys, gq, scores, giq, giw, kbuf,
    key_sem, own_sem, isend, irecv, wsend, wrecv, qsend, qrecv,
):
    me = lax.axis_index("seq")
    rows, span, _ = keys.shape
    half = n // 2
    partner = me + 1 - 2 * lax.rem(me, 2)
    order = sorted(range(1, half), key=lambda k: min(k, half - k))
    loads = []
    for b in range(rows):
        copy = pltpu.make_async_copy(keys.at[b], kbuf.at[b], key_sem.at[b])
        copy.start()
        loads.append(copy)
    own = [
        pltpu.make_async_copy(iq, giq.at[me], own_sem.at[0]),
        pltpu.make_async_copy(iw, giw.at[me], own_sem.at[1]),
        pltpu.make_async_copy(lq, gq.at[me], own_sem.at[2]),
    ]
    for copy in own:
        copy.start()
    greet_all(n, me)

    def push(peer, k, src, dst, send_sem, recv_sem):
        return pltpu.make_async_remote_copy(
            src_ref=src,
            dst_ref=dst,
            send_sem=send_sem.at[k],
            recv_sem=recv_sem.at[k],
            device_id={"seq": peer},
            device_id_type=MESH,
        )

    def first_hop(src, dst, send_sem, recv_sem):
        away = {
            k: push(lax.rem(me + 2 * k, n), k, src, dst.at[me], send_sem, recv_sem)
            for k in order
        }
        return away, push(partner, half, src, dst.at[me], send_sem, recv_sem)

    def second_hop(dst, send_sem, recv_sem):
        passed = {}
        for k in order:
            owner = lax.rem(me - 2 * k + n, n)
            passed[k] = push(
                partner, half + k, dst.at[owner], dst.at[owner], send_sem, recv_sem
            )
        return passed

    small = []
    for k in range(1, n):
        peer = lax.rem(me + k, n)
        small.append(push(peer, k, iq, giq.at[me], isend, irecv))
        small.append(push(peer, k, iw, giw.at[me], wsend, wrecv))
    (large, large_pair), large_on = first_hop(lq, gq, qsend, qrecv), second_hop(gq, qsend, qrecv)
    for copy in small:
        copy.start()
    for k in order:
        large[k].start()
    large_pair.start()
    for copy in loads:
        copy.wait()
    own[0].wait()
    own[1].wait()
    for copy in small:
        copy.wait_recv()
    tile = min(512, span)
    lane = lax.broadcasted_iota(jnp.int32, (1, tile), 1)
    held = giq.shape[2]
    given = iw.shape[1]
    diagonal = (
        lax.broadcasted_iota(jnp.int32, (n * held, given), 0) % held
        == lax.broadcasted_iota(jnp.int32, (n * held, given), 1)
    )
    waiting = list(order)
    for b in range(rows):
        query = giq[:, b].astype(jnp.float32).reshape(n * held, giq.shape[3])
        query = query.astype(jnp.bfloat16)
        weight = giw[:, b : b + 1].astype(jnp.float32)
        weight = jnp.broadcast_to(weight, (n, held, given)).reshape(n * held, given)
        weight = jnp.sum(jnp.where(diagonal, weight, 0.0), axis=1, keepdims=True)
        weight = jnp.broadcast_to(weight * IDX_DIM ** (-0.5), (n * held, LANES))
        length = lens[b]

        def step(c, carry, b=b, query=query, weight=weight, length=length):
            start = pl.multiple_of(c * tile, tile)
            dots = lax.dot_general(
                query,
                kbuf[b, pl.ds(start, tile), :],
                (((1,), (1,)), ((), ())),
                preferred_element_type=jnp.float32,
            )
            pieces = []
            for j in range(tile // LANES):
                part = jnp.maximum(dots[:, j * LANES : (j + 1) * LANES], 0.0) * weight
                pieces.append(jnp.sum(part, axis=0, keepdims=True))
            total = jnp.concatenate(pieces, axis=1)
            live = me * span + c * tile + lane < length
            scores[b : b + 1, pl.ds(start, tile)] = jnp.where(live, total, 0.0)
            return carry

        lax.fori_loop(0, span // tile, step, 0)
        if waiting:
            k = waiting.pop(0)
            large[k].wait_recv()
            large_on[k].start()
    for k in waiting:
        large[k].wait_recv()
        large_on[k].start()
    own[2].wait()
    large_pair.wait_recv()
    for k in order:
        large_on[k].wait_recv()
    for copy in small:
        copy.wait_send()
    large_pair.wait_send()
    for k in order:
        large[k].wait_send()
        large_on[k].wait_send()


def local_kernel(sel, lens, gq, cache, parts, stats, buf, counts, kept, sems):
    me = lax.axis_index("seq")
    rows, width, span = cache.shape
    nsel = sel.shape[2]
    here = span // BLOCK
    first = me * here

    def block_copy(b, rg, block, slot):
        start = pl.multiple_of((block - first) // 2 * LANES, LANES)
        dest = pl.multiple_of(slot * LANES, LANES)
        return pltpu.make_async_copy(
            cache.at[b, :, pl.ds(start, LANES)],
            buf.at[rg, :, pl.ds(dest, LANES)],
            sems.at[rg, slot],
        )

    for b in range(rows):
        for g in range(HEAD_GROUPS):
            rg = b * HEAD_GROUPS + g

            def scan(i, slot, b=b, g=g, rg=rg):
                block = sel[b, g, i]
                kept[rg, slot] = block
                mine = jnp.logical_and(block >= first, block < first + here)
                return slot + mine.astype(jnp.int32)

            count = lax.fori_loop(0, nsel, scan, jnp.int32(0), unroll=True)
            counts[rg] = count

            @pl.loop(0, count)
            def _(slot, b=b, rg=rg):
                block_copy(b, rg, kept[rg, slot], slot).start()

    for rg in range(rows * HEAD_GROUPS):
        count = counts[rg]

        @pl.loop(count, jnp.maximum((count + CHUNK - 1) // CHUNK, 1) * CHUNK)
        def _(slot, rg=rg):
            dest = pl.multiple_of(slot * LANES, LANES)
            buf[rg, :, pl.ds(dest, LANES)] = jnp.zeros((width, LANES), jnp.bfloat16)

    heads = gq.shape[2]
    per_group = gq.shape[0] // HEAD_GROUPS
    group_wise = per_group * heads
    tokens = CHUNK * LANES
    scale = (VALUE_WIDTH + ROTARY_WIDTH) ** (-0.5)
    lane = lax.broadcasted_iota(jnp.int32, (1, LANES), 1)
    for g in range(HEAD_GROUPS):
        table = jnp.zeros((group_wise, LANES), jnp.float32)
        for b in range(rows):
            rg = b * HEAD_GROUPS + g
            count = counts[rg]
            steps = jnp.maximum((count + CHUNK - 1) // CHUNK, 1)

            @pl.loop(0, count)
            def _(slot, b=b, rg=rg):
                block_copy(b, rg, first, slot).wait()

            query = gq[g * per_group : (g + 1) * per_group, b].reshape(group_wise, width)

            def chunk(c, b=b, rg=rg, query=query, count=count):
                base = pl.multiple_of(c * tokens, tokens)
                s = jnp.dot(
                    query,
                    buf[rg, :, pl.ds(base, tokens)],
                    preferred_element_type=jnp.float32,
                ) * scale
                bounds = []
                for j in range(CHUNK):
                    slot = c * CHUNK + j
                    block = kept[rg, slot]
                    begin = block % 2 * BLOCK
                    live = jnp.minimum(BLOCK, lens[b] - block * BLOCK)
                    bounds.append((begin, jnp.where(slot < count, begin + live, 0)))
                usable = jnp.concatenate(
                    [
                        ((lane >= lo) & (lane < hi)).astype(jnp.int32)
                        for lo, hi in bounds
                    ],
                    axis=1,
                ) > 0
                s = jnp.where(usable, s, NEG)
                return s, usable, buf[rg, :LATENT_WIDTH, pl.ds(base, tokens)]

            def mix(p, values):
                return lax.dot_general(
                    p.astype(jnp.bfloat16),
                    values,
                    (((1,), (1,)), ((), ())),
                    preferred_element_type=jnp.float32,
                )

            s, usable, values = chunk(0)
            top = jnp.max(s, axis=1, keepdims=True)
            p = jnp.where(usable, jnp.exp(s - top), 0.0)
            total = jnp.sum(p, axis=1, keepdims=True)
            acc = mix(p, values)

            def more(c, carry, chunk=chunk):
                top, total, acc = carry
                s, usable, values = chunk(c)
                new = jnp.maximum(top, jnp.max(s, axis=1, keepdims=True))
                p = jnp.where(usable, jnp.exp(s - new), 0.0)
                keep = jnp.exp(top - new)
                total = total * keep + jnp.sum(p, axis=1, keepdims=True)
                return new, total, acc * keep + mix(p, values)

            top, total, acc = lax.fori_loop(1, steps, more, (top, total, acc))
            parts[g * per_group : (g + 1) * per_group, b] = acc.astype(jnp.bfloat16).reshape(
                per_group, heads, LATENT_WIDTH
            )
            table = jnp.where(lane == 2 * b, top, table)
            table = jnp.where(lane == 2 * b + 1, total, table)
        stats[g * per_group : (g + 1) * per_group] = table.reshape(per_group, heads, LANES)


def exchange_kernel(
    n, parts, stats, weight, out, rparts, rstats, wbuf,
    own_sem, psend, precv, ssend, srecv,
):
    me = lax.axis_index("seq")
    _, rows, heads, latent = parts.shape
    own = [
        pltpu.make_async_copy(weight, wbuf, own_sem.at[0]),
        pltpu.make_async_copy(parts.at[me], rparts.at[me], own_sem.at[1]),
        pltpu.make_async_copy(stats.at[me], rstats.at[me], own_sem.at[2]),
    ]
    for copy in own:
        copy.start()
    greet_all(n, me)
    sends = []
    for k in range(1, n):
        peer = lax.rem(me + k, n)
        sends.append(push(n, me, k, stats.at[peer], rstats.at[me], ssend, srecv))
        sends.append(push(n, me, k, parts.at[peer], rparts.at[me], psend, precv))
    for copy in sends:
        copy.start()
    for copy in own:
        copy.wait()
    for copy in sends:
        copy.wait_recv()
    table = rstats[...]
    attended = []
    for b in range(rows):
        tops = [table[s, :, 2 * b : 2 * b + 1] for s in range(n)]
        joint = functools.reduce(jnp.maximum, tops)
        total = jnp.zeros_like(joint)
        acc = jnp.zeros((heads, latent), jnp.float32)
        for s in range(n):
            factor = jnp.exp(tops[s] - joint)
            total = total + factor * table[s, :, 2 * b + 1 : 2 * b + 2]
            acc = acc + factor * rparts[s, b].astype(jnp.float32)
        attended.append(acc / total)
    attended = jnp.concatenate(attended, axis=0).astype(jnp.bfloat16)
    which = lax.broadcasted_iota(jnp.int32, (rows * heads, 1), 0) % heads

    def project(h, acc):
        y = jnp.dot(attended, wbuf[h], preferred_element_type=jnp.float32)
        return jnp.where(which == h, y, acc)

    y = jnp.zeros((rows * heads, weight.shape[2]), jnp.float32)
    y = lax.fori_loop(0, heads, project, y, unroll=4)
    out[...] = y.reshape(rows, heads, weight.shape[2]).astype(out.dtype)
    for copy in sends:
        copy.wait_send()


def on_device(
    n,
    latent_cache,
    index_keys,
    latent_query,
    index_query,
    index_weight,
    value_up_weight,
    selected,
    lengths,
):
    cache, keys, lq = latent_cache[0], index_keys[0], latent_query[0]
    iq, iw, weight, sel = index_query[0], index_weight[0], value_up_weight[0], selected[0]
    rows, span, width = cache.shape
    heads = lq.shape[1]
    extra = -iq.shape[1] % 8
    if extra:
        iq = jnp.pad(iq, ((0, 0), (0, extra), (0, 0)))
    vmem = pl.BlockSpec(memory_space=pltpu.VMEM)
    smem = pl.BlockSpec(memory_space=pltpu.SMEM)
    hbm = pl.BlockSpec(memory_space=pl.ANY)
    dma = pltpu.SemaphoreType.DMA
    limit = 60 * 1024 * 1024

    gq, index_scores = pl.pallas_call(
        functools.partial(gather_kernel, n),
        out_shape=(
            jax.ShapeDtypeStruct((n,) + lq.shape, lq.dtype),
            jax.ShapeDtypeStruct((rows, span), jnp.float32),
        ),
        in_specs=[smem, vmem, vmem, vmem, hbm],
        out_specs=(hbm, vmem),
        scratch_shapes=[
            pltpu.VMEM((n,) + iq.shape, iq.dtype),
            pltpu.VMEM((n,) + iw.shape, iw.dtype),
            pltpu.VMEM(keys.shape, keys.dtype),
            dma((rows,)), dma((3,)), dma((n,)), dma((n,)), dma((n,)), dma((n,)),
            dma((n,)), dma((n,)),
        ],
        compiler_params=pltpu.CompilerParams(
            collective_id=0, has_side_effects=True, vmem_limit_bytes=limit
        ),
        name="gather",
    )(lengths, lq, iq, iw, keys)

    whole_heads = n * heads
    if heads % 16:
        gq = gq.transpose(1, 0, 2, 3).reshape(
            rows, HEAD_GROUPS, whole_heads // HEAD_GROUPS, width
        ).transpose(1, 0, 2, 3)
    slots = gq.shape[0]
    wide = gq.shape[2]
    pairs = rows * HEAD_GROUPS
    nsel = sel.shape[2]
    room = -(-nsel // CHUNK) * CHUNK
    parts, stats = pl.pallas_call(
        local_kernel,
        out_shape=(
            jax.ShapeDtypeStruct((slots, rows, wide, LATENT_WIDTH), jnp.bfloat16),
            jax.ShapeDtypeStruct((slots, wide, 128), jnp.float32),
        ),
        in_specs=[smem, smem, vmem, hbm],
        out_specs=(vmem, vmem),
        scratch_shapes=[
            pltpu.VMEM((pairs, width, room * LANES), cache.dtype),
            pltpu.SMEM((pairs,), jnp.int32),
            pltpu.SMEM((pairs, room), jnp.int32),
            dma((pairs, nsel)),
        ],
        compiler_params=pltpu.CompilerParams(vmem_limit_bytes=limit),
        name="local",
    )(sel, lengths, gq, jnp.swapaxes(cache, 1, 2))
    if slots != n:
        parts = parts.transpose(1, 0, 2, 3).reshape(rows, n, heads, LATENT_WIDTH)
        parts = parts.transpose(1, 0, 2, 3)
        stats = stats.reshape(n, heads, 128)

    head_out = pl.pallas_call(
        functools.partial(exchange_kernel, n),
        out_shape=jax.ShapeDtypeStruct((rows, heads, weight.shape[2]), jnp.float32),
        in_specs=[hbm, hbm, hbm],
        out_specs=vmem,
        scratch_shapes=[
            pltpu.VMEM(parts.shape, parts.dtype),
            pltpu.VMEM(stats.shape, stats.dtype),
            pltpu.VMEM(weight.shape, weight.dtype),
            dma((3,)), dma((n,)), dma((n,)), dma((n,)), dma((n,)),
        ],
        compiler_params=pltpu.CompilerParams(
            collective_id=1, has_side_effects=True, vmem_limit_bytes=limit
        ),
        name="exchange",
    )(parts, stats, weight)
    return (index_scores[None], head_out.astype(jnp.bfloat16)[None])


def solution(mesh):
    return jax.shard_map(
        functools.partial(on_device, mesh.shape["seq"]),
        mesh=mesh,
        in_specs=(
            P("section", "groups", "seq", None),
            P("section", "groups", "seq", None),
            P("section", "groups", "seq", None),
            P("section", "groups", "seq", None),
            P("section", "groups", "seq"),
            P("section", "seq", None, None),
            P("section", "groups", None, None),
            P("groups"),
        ),
        out_specs=(P("section", "groups", "seq"), P("section", "groups", "seq", None)),
        check_vma=False,
    )
```
